32 devices in a mesh: space: 4 (over y, x), dp: 8 (over z, core).
Axes of the slice: x: 2, y: 2, z: 4, core: 2. Of those that a mesh axis runs over, the one named last changes fastest.
Arguments:
- mixed_two: bfloat16 [8, 16, 180, 768], P('dp', 'space'), may hold values from -6 to 6
- input_two: bfloat16 [8, 16, 180, 768], P('dp', 'space'), may hold values from -6 to 6
- cotangent: bfloat16 [8, 16, 180, 768], P('dp', 'space'), may hold values from -6 to 6
- w_in_two: bfloat16 [3072, 768], replicated, may hold values from -0.21875 to 0.21875
- w_out_two: bfloat16 [3072, 768], replicated, may hold values from -0.109375 to 0.109375
- kernel_two: bfloat16 [9, 768], replicated, may hold values from -2 to 2
- mixed_one: bfloat16 [8, 16, 180, 768], P('dp', 'space'), may hold values from -6 to 6
- w_in_one: bfloat16 [3072, 768], replicated, may hold values from -0.21875 to 0.21875
- w_out_one: bfloat16 [3072, 768], replicated, may hold values from -0.109375 to 0.109375
- kernel_one: bfloat16 [9, 768], replicated, may hold values from -2 to 2
Outputs:
- input_grad: bfloat16 [8, 16, 180, 768], P('dp', 'space')
- grad_w_in: float32 [3072, 768], P('dp')
- grad_w_out: float32 [3072, 768], P('dp')
- grad_kernel: float32 [9, 768], replicated
The draws below stay inside these ranges and needn't reach their ends.
All inputs are finite; a program needn't handle non-finite values.
Results may differ from the reference program's by a relative error of at most 0.02.
Values may be sent and summed in bfloat16 or wider, within the bound.
A program may use at most 192 MiB of HBM per device.

```python
import math
import jax
import jax.numpy as jnp
from jax import lax

D = 768
FF = 3072
LON = 180
LAT = 16
BATCH = 8
TAPS = 9


def shard_levels(stream_key, extent, cuts, smallest, top_value):
    loudness = 1.0
    for dim, parts in cuts:
        steps = jax.random.uniform(jax.random.fold_in(jax.random.fold_in(stream_key, 6), dim), (parts,), jnp.float32, smallest / len(cuts), top_value / len(cuts))
        loudness = loudness * jnp.repeat(jnp.exp(steps), extent[dim] // parts).reshape((-1,) + (1,) * (len(extent) - 1 - dim))
    return loudness


def bell_draw(key, dims, width, limit, shards=(), held_as=jnp.bfloat16):
    drawn = jax.random.normal(key, dims, jnp.float32) * width
    if len(shards) > 0:
        drawn = shard_levels(key, dims, shards, -0.22, 0.18) * drawn
    return jnp.clip(drawn, min=-limit, max=limit).astype(held_as)


def setup_inputs(seed: int = 0) -> dict:
    seeds = jax.random.split(jax.random.key(seed), 11)
    mixed_two = bell_draw(seeds[0], (BATCH, LAT, LON, D), 1.0, 6.0, ((0, 8), (1, 4)))
    input_two = bell_draw(seeds[1], (BATCH, LAT, LON, D), 1.0, 6.0, ((0, 8), (1, 4)))
    cotangent = bell_draw(seeds[2], (BATCH, LAT, LON, D), 1.0, 6.0, ((0, 8), (1, 4)))
    w_in_two = bell_draw(seeds[3], (FF, D), D ** -0.5, 0.21875)
    w_out_two = bell_draw(seeds[4], (FF, D), FF ** -0.5, 0.109375)
    kernel_two = bell_draw(seeds[5], (TAPS, D), 0.35, 2.0)
    mixed_one = bell_draw(seeds[6], (BATCH, LAT, LON, D), 1.0, 6.0, ((0, 8), (1, 4)))
    w_in_one = bell_draw(seeds[7], (FF, D), D ** -0.5, 0.21875)
    w_out_one = bell_draw(seeds[8], (FF, D), FF ** -0.5, 0.109375)
    kernel_one = bell_draw(seeds[9], (TAPS, D), 0.35, 2.0)
    return {"mixed_two": mixed_two, "input_two": input_two, "cotangent": cotangent, "w_in_two": w_in_two, "w_out_two": w_out_two, "kernel_two": kernel_two, "mixed_one": mixed_one, "w_in_one": w_in_one, "w_out_one": w_out_one, "kernel_one": kernel_one}


GELU_C = math.sqrt(2.0 / math.pi)
CONTRACT_LAST = (((1,), (1,)), ((), ()))
CONTRACT_FIRST = (((0,), (0,)), ((), ()))

def gelu_parts(preact):
    tanh_arg = GELU_C * (preact + 0.044715 * preact * preact * preact)
    tanh_val = jnp.tanh(tanh_arg)
    activation = 0.5 * preact * (1.0 + tanh_val)
    gelu_slope = 0.5 * (1.0 + tanh_val) + 0.5 * preact * (1.0 - tanh_val * tanh_val) * GELU_C * (1.0 + 3.0 * 0.044715 * preact * preact)
    return (activation, gelu_slope)

def pad_rows(field):
    return jnp.pad(field, ((0, 0), (1, 1), (0, 0), (0, 0)))

def conv_back(padded, kernel, band_rows):
    kernel_f = kernel.astype(jnp.float32)
    result = jnp.zeros(padded[:, 1:1 + band_rows].shape, jnp.float32)
    for lat_off in range(3):
        for lon_off in range(3):
            window = padded[:, 2 - lat_off:2 - lat_off + band_rows].astype(jnp.float32)
            result = result + kernel_f[3 * lat_off + lon_off] * jnp.roll(window, lon_off - 1, axis=2)
    return result

def kernel_terms(padded_in, mix_grad, band_rows):
    grad_f = mix_grad.astype(jnp.float32)
    collected = []
    for lat_off in range(3):
        for lon_off in range(3):
            window = jnp.roll(padded_in[:, lat_off:lat_off + band_rows], 1 - lon_off, axis=2)
            collected.append(lax.optimization_barrier(jnp.sum(window.astype(jnp.float32) * grad_f, axis=(0, 1, 2))))
    return jnp.stack(collected)

def reference(mixed_two, input_two, cotangent, w_in_two, w_out_two, kernel_two, mixed_one, w_in_one, w_out_one, kernel_one):

    def sample_pass(items):
        mixed_late, input_late, cot_late, mixed_early = [item[None] for item in items]
        shape4 = mixed_late.shape
        band_rows = shape4[1]
        channels = shape4[3]
        mixed_flat = mixed_late.reshape(-1, channels)
        cot_flat = cot_late.reshape(-1, channels)
        preact = lax.dot_general(mixed_flat, w_in_two, CONTRACT_LAST, preferred_element_type=jnp.float32)
        activation, gelu_slope = gelu_parts(preact)
        activation = activation.astype(jnp.bfloat16)
        hidden_grad = lax.dot_general(cot_flat, w_out_two, CONTRACT_LAST, preferred_element_type=jnp.float32)
        pre_grad = (hidden_grad * gelu_slope).astype(jnp.bfloat16)
        mix_grad = jnp.dot(pre_grad, w_in_two, preferred_element_type=jnp.float32).astype(jnp.bfloat16).reshape(shape4)
        out_term = lax.dot_general(activation, cot_flat, CONTRACT_FIRST, preferred_element_type=jnp.float32)
        in_term = lax.dot_general(pre_grad, mixed_flat, CONTRACT_FIRST, preferred_element_type=jnp.float32)
        taps_term = kernel_terms(pad_rows(input_late), mix_grad, band_rows)
        grad_two = (cot_late.astype(jnp.float32) + conv_back(pad_rows(mix_grad), kernel_two, band_rows)).astype(jnp.bfloat16)
        preact_early = lax.dot_general(mixed_early.reshape(-1, channels), w_in_one, CONTRACT_LAST, preferred_element_type=jnp.float32)
        unused_act, slope_early = gelu_parts(preact_early)
        hidden_early = lax.dot_general(grad_two.reshape(-1, channels), w_out_one, CONTRACT_LAST, preferred_element_type=jnp.float32)
        pre_early = (hidden_early * slope_early).astype(jnp.bfloat16)
        mix_early = jnp.dot(pre_early, w_in_one, preferred_element_type=jnp.float32).astype(jnp.bfloat16).reshape(shape4)
        grad_one = (grad_two.astype(jnp.float32) + conv_back(pad_rows(mix_early), kernel_one, band_rows)).astype(jnp.bfloat16)
        return (grad_one[0], in_term, out_term, taps_term)
    grad_one, in_terms, out_terms, tap_terms = lax.map(sample_pass, (mixed_two, input_two, cotangent, mixed_one))
    grad_w_in = lax.optimization_barrier(jnp.sum(in_terms, axis=0)) / BATCH
    grad_w_out = lax.optimization_barrier(jnp.sum(out_terms, axis=0)) / BATCH
    grad_kernel = lax.optimization_barrier(jnp.sum(tap_terms, axis=0)) / BATCH
    return (grad_one, grad_w_in, grad_w_out, grad_kernel)
```

```python
import functools
import math

import jax
import jax.numpy as jnp
from jax import lax
from jax.experimental import pallas as pl
from jax.experimental.pallas import tpu as pltpu
from jax.sharding import PartitionSpec as P

MESH = pl.DeviceIdType.MESH
F32 = jnp.float32
BF16 = jnp.bfloat16
GELU_C = math.sqrt(2.0 / math.pi)
GELU_D = 0.044715 * GELU_C
NT = (((1,), (1,)), ((), ()))
NN = (((1,), (0,)), ((), ()))
TN = (((0,), (0,)), ((), ()))
LANES = 128
STREAMS = 3
COMM = True


def dot(a, b, dims):
    return lax.dot_general(a, b, dims, preferred_element_type=F32)


def gelu_slope_parts(v):
    cube = GELU_D * (v * v)
    t = jnp.tanh(v * (cube + GELU_C))
    p = 1.0 + t
    act = (0.5 * v) * p
    slope = 0.5 * p + act * (1.0 - t) * (3.0 * cube + GELU_C)
    return act, slope


def bits_of(n):
    return (n - 1).bit_length()


def my_bit(index, bit):
    return (index // (1 << bit)) % 2


def flip(index, bit):
    return index + (1 << bit) * (1 - 2 * my_bit(index, bit))


def rolled(row, shift):
    if shift == 0:
        return row
    if shift == 1:
        return jnp.concatenate([row[-1:], row[:-1]], axis=0)
    return jnp.concatenate([row[1:], row[:1]], axis=0)


class Plan:
    def __init__(self, dp, space, hidden, width):
        self.dp, self.space = dp, space
        self.db, self.sb = bits_of(dp), bits_of(space)
        self.width = width
        rows = hidden // (dp * space)
        self.piece = next(q for q in (16, 8, rows) if rows % q == 0)
        self.chunks = rows // self.piece
        self.lanes = width // STREAMS
        spaces = [("space", b) for b in range(self.sb)]
        rest = [("dp", b) for b in range(1, self.db)]
        self.orders = [spaces + rest, spaces[::-1] + rest, rest + spaces]
        self.stages = self.sb + self.db - 1

    def labels(self):
        return [("dp", b) for b in reversed(range(self.db))] + [
            ("space", b) for b in reversed(range(self.sb))
        ]


def kernel(
    plan, shape, inv_batch,
    mixed_two, input_two, cotangent, w_in_two, w_out_two, kernel_two, mixed_one, w_in_one, w_out_one, kernel_one,
    out_ref, grads_ref, taps_out,
    raw_mixed, raw_input, raw_cot, raw_one,
    mixed, cot, early, w_in, w_out, w_late, act_t, pg_t, mix_acc, mix_row, grad_two, slope,
    halo_late, halo_early, taps, taps_in, term, final, *rest,
):
    stage_in = rest[: plan.stages + 1]
    (
        load_sem, weight_sem, late_sem, out_sem, own_sem,
        send_sem, recv_sem, gsend_sem, grecv_sem, hsend_sem, hrecv_sem, tsend_sem, trecv_sem,
    ) = rest[plan.stages + 1 :]
    rows, cols, width = shape
    pad = mixed.shape[1]
    tokens = rows * pad
    K = plan.chunks
    F = w_in.shape[0] * w_in.shape[2]
    dpi, spi = lax.axis_index("dp"), lax.axis_index("space")
    where = {"dp": dpi, "space": spi}
    labels = plan.labels()
    order = [0, rows - 1] + list(range(1, rows - 1))
    place = {r: n for n, r in enumerate(order)}

    loads = [
        pltpu.make_async_copy(src.at[0], dst, load_sem.at[n])
        for n, (src, dst) in enumerate(
            [(mixed_two, raw_mixed), (cotangent, raw_cot), (mixed_one, raw_one), (input_two, raw_input)]
        )
    ]

    def weight_load(k, which):
        src, dst = ((w_in_two, w_in), (w_out_two, w_out))[which]
        return pltpu.make_async_copy(src.at[:, k], dst.at[:, k], weight_sem.at[which, k])

    late_loads = [
        pltpu.make_async_copy(w_in_one, w_late, late_sem.at[0]),
        pltpu.make_async_copy(w_out_one, w_out, late_sem.at[1]),
    ]
    loads[0].start()
    weight_load(0, 0).start()
    loads[1].start()
    weight_load(0, 1).start()
    for k in range(1, K):
        weight_load(k, 0).start()
        weight_load(k, 1).start()
    loads[2].start()
    loads[3].start()
    late_loads[0].start()

    peers = [{"dp": flip(dpi, b)} for b in range(plan.db)]

    def across(offset):
        other = spi
        for b in range(plan.sb):
            if (offset >> b) & 1:
                other = flip(other, b)
        return other

    peers += [{"space": across(o)} for o in range(1, plan.space)]
    if COMM:
        barrier = pltpu.get_barrier_semaphore()
        for peer in peers:
            pl.semaphore_signal(barrier, inc=1, device_id=peer, device_id_type=MESH)

    zeros = jnp.zeros((16, width), BF16)
    for r in range(rows):
        mixed[r, pl.ds(pad - 16, 16)] = zeros
        cot[r, pl.ds(pad - 16, 16)] = zeros
        early[r, pl.ds(pad - 16, 16)] = zeros
        grad_two[r, pl.ds(pad - 16, 16)] = zeros
    mix_acc[...] = jnp.zeros_like(mix_acc)
    for halo in (halo_late, halo_early):
        pl.when(spi == 0)(lambda halo=halo: halo.__setitem__(0, jnp.zeros(halo.shape[1:], BF16)))
        pl.when(spi == plan.space - 1)(lambda halo=halo: halo.__setitem__(1, jnp.zeros(halo.shape[1:], BF16)))

    if COMM:
        pl.semaphore_wait(barrier, len(peers))

    loads[0].wait()
    for r in range(rows):
        mixed[r, pl.ds(0, cols)] = raw_mixed[r]
    loads[1].wait()
    for r in range(rows):
        cot[r, pl.ds(0, cols)] = raw_cot[r]

    def half(done, now, value):
        index = []
        for label in labels:
            if label in done:
                index.append(my_bit(where[label[0]], label[1]))
            elif label == now:
                index.append(value)
            else:
                index.append(slice(None))
        return tuple(index)

    def exchange(k, stage, stream):
        if stage == 0:
            now, done, streams = ("dp", 0), [], slice(None)
            dst = stage_in[0].at[k]
        else:
            now = plan.orders[stream][stage - 1]
            done, streams = [("dp", 0)] + plan.orders[stream][: stage - 1], stream
            dst = stage_in[stage].at[k, stream]
        mine = my_bit(where[now[0]], now[1])
        src = term.at[(k, streams, slice(None)) + half(done, now, 1 - mine)]
        kept = (k, streams, slice(None)) + half(done, now, mine)
        copy = pltpu.make_async_remote_copy(
            src_ref=src,
            dst_ref=dst,
            send_sem=send_sem.at[k, stage, stream],
            recv_sem=recv_sem.at[k, stage, stream],
            device_id={now[0]: flip(where[now[0]], now[1])},
            device_id_type=MESH,
        )
        return copy, kept, dst

    def gather(k, offset):
        return pltpu.make_async_remote_copy(
            src_ref=final.at[k],
            dst_ref=grads_ref.at[k, spi],
            send_sem=gsend_sem.at[k, offset - 1],
            recv_sem=grecv_sem.at[k, offset - 1],
            device_id={"space": across(offset)},
            device_id_type=MESH,
        )

    def own(k):
        return pltpu.make_async_copy(final.at[k], grads_ref.at[k, spi], own_sem.at[k])

    def streams_of(stage):
        return range(1 if stage == 0 else STREAMS)

    def start(k, stage):
        if not COMM:
            return
        for stream in streams_of(stage):
            exchange(k, stage, stream)[0].start()

    def finish(k, stage):
        if not COMM:
            return
        last = stage == plan.stages
        for stream in streams_of(stage):
            copy, kept, came = exchange(k, stage, stream)
            copy.wait()
            if stage == 0:
                for s in range(STREAMS):
                    for a in range(2):
                        index = (k, s, a) + kept[3:]
                        total = term[index].astype(F32) + stage_in[0][k, s, a].astype(F32)
                        term[index] = total.astype(BF16)
            else:
                total = (term[kept].astype(F32) + came[...].astype(F32)).astype(BF16)
                if last:
                    final[k, :, :, pl.ds(stream * plan.lanes, plan.lanes)] = total
                else:
                    term[kept] = total
            if not last and stage > 0:
                exchange(k, stage + 1, stream)[0].start()
        if stage == 0:
            start(k, 1)
        if last:
            for offset in range(1, plan.space):
                gather(k, offset).start()
            own(k).start()

    def tick(i, static):
        for stage in reversed(range(plan.stages + 1)):
            k = i - 1 - stage
            if static:
                if 0 <= k < K:
                    finish(k, stage)
            else:
                pl.when(k >= 0)(functools.partial(finish, k, stage))

    def late_chunk(k, carry):
        weight_load(k, 0).wait()
        weight_load(k, 1).wait()

        wi = w_in[:, k].reshape(F, width)
        wo = w_out[:, k].reshape(F, width)

        def tile(t, c):
            first = pl.multiple_of(t * pad, pad)
            v = dot(wi, mixed[t], NT)
            h = dot(wo, cot[t], NT)
            act, grad = gelu_slope_parts(v)
            act_t[t] = act.astype(BF16)
            pg_t[t] = (h * grad).astype(BF16)
            return c

        for t in range(rows):
            tile(t, 0)
        tick(k, False)

        def put(a, value):
            value = (value * inv_batch).astype(BF16)
            for s in range(STREAMS):
                part = value[:, s * plan.lanes : (s + 1) * plan.lanes]
                term[k, s, a] = part.reshape(term.shape[3:])

        def against(lhs, rhs):
            total = dot(lhs[0], rhs[0], NN)
            for t in range(1, rows):
                total = total + dot(lhs[t], rhs[t], NN)
            return total

        put(0, against(act_t, cot))
        put(1, against(pg_t, mixed))
        start(k, 0)
        for t in range(rows):
            mix_acc[t] += dot(pg_t[t], wi, TN)
        return carry

    lax.fori_loop(0, K, late_chunk, 0)
    late_loads[1].start()

    def halo_copy(rows_ref, halo, side, which):
        src = rows_ref.at[0 if side == 0 else rows - 1]
        return pltpu.make_async_remote_copy(
            src_ref=src,
            dst_ref=halo.at[1 - side],
            send_sem=hsend_sem.at[which, side],
            recv_sem=hrecv_sem.at[which, 1 - side],
            device_id={"space": spi - 1 if side == 0 else spi + 1},
            device_id_type=MESH,
        )

    def halo_do(rows_ref, halo, which, act):
        if not COMM:
            return
        pl.when(spi > 0)(lambda: act(halo_copy(rows_ref, halo, 0, which), 0))
        pl.when(spi < plan.space - 1)(lambda: act(halo_copy(rows_ref, halo, 1, which), 1))

    def halo_start(rows_ref, halo, which):
        halo_do(rows_ref, halo, which, lambda copy, side: copy.start())

    def halo_wait(rows_ref, halo, which):
        def wait(copy, side):
            copy.wait_send()
            pltpu.make_async_remote_copy(
                src_ref=rows_ref.at[0],
                dst_ref=halo.at[side],
                send_sem=hsend_sem.at[which, side],
                recv_sem=hrecv_sem.at[which, side],
                device_id={"space": spi - 1 if side == 0 else spi + 1},
                device_id_type=MESH,
            ).wait_recv()

        halo_do(rows_ref, halo, which, wait)

    for r in range(rows):
        mix_row[r] = mix_acc[r].astype(BF16)
    halo_start(mix_row, halo_late, 0)
    tick(K, True)
    ticks = iter(range(K + 1, K + plan.stages + 1))

    def next_tick():
        i = next(ticks, None)
        if i is not None:
            tick(i, True)

    def conv(wanted, halo, rows_ref, kernel_ref, base, store, with_taps):
        def block(c, carry):
            lanes = pl.ds(pl.multiple_of(c * LANES, LANES), LANES)
            weights = kernel_ref[:, lanes].astype(F32)
            windows = {}
            sums = [None] * 9
            for i in wanted:
                total = base(i, lanes).astype(F32)
                held = raw_input[i, :, lanes].astype(F32) if with_taps else None
                for lat in range(3):
                    p = i + 2 - lat
                    if p not in windows:
                        if p == 0:
                            row = halo[0, pl.ds(0, cols), lanes]
                        elif p == rows + 1:
                            row = halo[1, pl.ds(0, cols), lanes]
                        else:
                            row = rows_ref[p - 1, pl.ds(0, cols), lanes]
                        windows[p] = [rolled(row.astype(F32), b - 1) for b in range(3)]
                    for lon in range(3):
                        tap = 3 * lat + lon
                        total = total + weights[tap : tap + 1] * windows[p][lon]
                        if with_taps:
                            part = jnp.sum(held * windows[p][lon], axis=0, keepdims=True)
                            sums[tap] = part if sums[tap] is None else sums[tap] + part
                store(i, lanes, total.astype(BF16))
            if with_taps:
                for tap in range(9):
                    taps[tap : tap + 1, lanes] += sums[tap]
            return carry

        lax.fori_loop(0, width // LANES, block, 0)

    loads[2].wait()
    for r in range(rows):
        early[place[r], pl.ds(0, cols)] = raw_one[r]
    late_loads[0].wait()
    hidden = w_late.shape[0]
    E = slope.shape[2]
    steps = hidden // E

    def early_slope(n, carry):
        w = w_late[pl.ds(pl.multiple_of(n * E, E), E)]
        for r in range(rows):
            v = dot(early[r], w, NT)
            slope[n, pl.ds(r * pad, pad)] = gelu_slope_parts(v)[1].astype(BF16)
        return carry

    lax.fori_loop(0, steps // 2, early_slope, 0)
    next_tick()
    lax.fori_loop(steps // 2, steps, early_slope, 0)
    next_tick()
    loads[3].wait()
    taps[...] = jnp.zeros_like(taps)

    def late_base(i, lanes):
        return raw_cot[i, :, lanes]

    def late_store(i, lanes, value):
        grad_two[place[i], pl.ds(0, cols), lanes] = value

    conv(range(1, rows - 1), halo_late, mix_row, kernel_two, late_base, late_store, True)
    halo_wait(mix_row, halo_late, 0)
    conv([0, rows - 1], halo_late, mix_row, kernel_two, late_base, late_store, True)
    taps[...] = taps[...] * inv_batch

    moves = [("dp", b) for b in range(plan.db)] + [("space", b) for b in range(plan.sb)]

    def taps_copy(n):
        axis, bit = moves[n]
        return pltpu.make_async_remote_copy(
            src_ref=taps,
            dst_ref=taps_in.at[n],
            send_sem=tsend_sem.at[n],
            recv_sem=trecv_sem.at[n],
            device_id={axis: flip(where[axis], bit)},
            device_id_type=MESH,
        )

    def taps_step(n):
        if not COMM:
            return
        if 0 < n <= len(moves):
            taps_copy(n - 1).wait()
            taps[...] += taps_in[n - 1]
        if n < len(moves):
            taps_copy(n).start()

    taps_step(0)
    steps_taps = iter(range(1, len(moves) + 1))

    def next_taps():
        n = next(steps_taps, None)
        if n is not None:
            taps_step(n)

    late_loads[1].wait()
    w_out_flat = w_out.reshape(hidden, width)

    def early_group(first, count):
        span = count * pad
        lo = first * pad

        def chunk(n, carry):
            w_o = w_out_flat[pl.ds(pl.multiple_of(n * E, E), E)]
            w_i = w_late[pl.ds(pl.multiple_of(n * E, E), E)]
            h = dot(grad_two[pl.ds(first, count)].reshape(span, width), w_o, NT)
            s = slope[n, pl.ds(lo, span)].astype(F32)
            g = (h * s).astype(BF16)
            back = dot(g, w_i, NN)
            for r in range(count):
                mix_acc[first + r] += back[r * pad : (r + 1) * pad]
            return carry

        for r in range(count):
            mix_acc[first + r] = jnp.zeros(mix_acc.shape[1:], F32)
        lax.fori_loop(0, steps // 2, chunk, 0)
        next_tick()
        next_taps()
        lax.fori_loop(steps // 2, steps, chunk, 0)
        for r in range(count):
            mix_row[order[first + r]] = mix_acc[first + r].astype(BF16)

    early_group(0, 2)
    halo_start(mix_row, halo_early, 1)
    next_tick()
    next_taps()
    early_group(2, rows - 2)
    next_tick()
    next_taps()

    def early_base(i, lanes):
        return grad_two[place[i], pl.ds(0, cols), lanes]

    def early_store(i, lanes, value):
        raw_mixed[i, :, lanes] = value

    def out_copy(i):
        return pltpu.make_async_copy(raw_mixed.at[i], out_ref.at[0, i], out_sem.at[i])

    conv(range(1, rows - 1), halo_early, mix_row, kernel_one, early_base, early_store, False)
    for i in range(1, rows - 1):
        out_copy(i).start()
    for _ in range(plan.stages):
        next_tick()
    halo_wait(mix_row, halo_early, 1)
    conv([0, rows - 1], halo_early, mix_row, kernel_one, early_base, early_store, False)
    out_copy(0).start()
    out_copy(rows - 1).start()
    for _ in moves:
        next_taps()
    taps_out[...] = taps[...]
    if COMM:
        for k in range(K):
            for offset in range(1, plan.space):
                gather(k, offset).wait()
            own(k).wait()
    for i in range(rows):
        out_copy(i).wait()


def whole_call(plan, inv_batch, args):
    mixed_two, input_two, cotangent, w_in_two, w_out_two, kernel_two, mixed_one, w_in_one, w_out_one, kernel_one = args
    _, rows, cols, width = mixed_two.shape
    hidden = w_in_two.shape[0]
    pad = -(-cols // 16) * 16
    K, dp, space, Q = plan.chunks, plan.dp, plan.space, plan.piece
    R = space * Q
    F = dp * R
    E = 512
    w_in_two = w_in_two.reshape(dp, K, R, width)
    w_out_two = w_out_two.reshape(dp, K, R, width)
    w_out_one = w_out_one.reshape(dp, K, R, width)
    anywhere = pl.BlockSpec(memory_space=pl.ANY)
    vmem = pl.BlockSpec(memory_space=pltpu.VMEM)
    stage_shapes = [
        pltpu.VMEM((K, STREAMS, 2) + (2,) * (plan.db + plan.sb - 1 - stage) + (Q, plan.lanes), BF16)
        for stage in range(plan.stages + 1)
    ]
    token = pltpu.VMEM((rows, pad, width), BF16)
    raw = pltpu.VMEM((rows, cols, width), BF16)
    taps = kernel_two.shape[0]
    moves = plan.db + plan.sb
    dma = pltpu.SemaphoreType.DMA
    scratch = [
        raw, raw, raw, raw,
        token, token, token,
        pltpu.VMEM((dp, K, R, width), BF16),
        pltpu.VMEM((dp, K, R, width), BF16),
        pltpu.VMEM((hidden, width), BF16),
        pltpu.VMEM((rows, F, pad), BF16),
        pltpu.VMEM((rows, F, pad), BF16),
        pltpu.VMEM((rows, pad, width), F32),
        token,
        token,
        pltpu.VMEM((hidden // E, rows * pad, E), BF16),
        pltpu.VMEM((2, pad, width), BF16),
        pltpu.VMEM((2, pad, width), BF16),
        pltpu.VMEM((taps, width), F32),
        pltpu.VMEM((moves, taps, width), F32),
        pltpu.VMEM((K, STREAMS, 2) + (2,) * moves + (Q, plan.lanes), BF16),
        pltpu.VMEM((K, 2, Q, width), BF16),
        *stage_shapes,
        dma((4,)), dma((2, K)), dma((2,)), dma((rows,)), dma((K,)),
        dma((K, plan.stages + 1, STREAMS)), dma((K, plan.stages + 1, STREAMS)),
        dma((K, space - 1)), dma((K, space - 1)),
        dma((2, 2)), dma((2, 2)), dma((moves,)), dma((moves,)),
    ]
    return pl.pallas_call(
        functools.partial(kernel, plan, (rows, cols, width), inv_batch),
        in_specs=[anywhere] * 5 + [vmem] + [anywhere] * 3 + [vmem],
        out_specs=[anywhere, anywhere, vmem],
        out_shape=[
            jax.ShapeDtypeStruct(mixed_two.shape, BF16),
            jax.ShapeDtypeStruct((K, space, 2, Q, width), BF16),
            jax.ShapeDtypeStruct((taps, width), F32),
        ],
        scratch_shapes=scratch,
        compiler_params=pltpu.CompilerParams(
            collective_id=0 if COMM else None, has_side_effects=True, vmem_limit_bytes=67_043_328
        ),
    )(mixed_two, input_two, cotangent, w_in_two, w_out_two, kernel_two, mixed_one, w_in_one, w_out_one, kernel_one)


def shards(*args):
    dp, space = lax.axis_size("dp"), lax.axis_size("space")
    samples, width, hidden = args[0].shape[0], args[0].shape[3], args[3].shape[0]
    plan = Plan(dp, space, hidden, width)
    grad_one, grads, taps = whole_call(plan, 1.0 / (samples * dp), args)
    out = grads[:, :, 0].reshape(-1, width).astype(F32)
    inn = grads[:, :, 1].reshape(-1, width).astype(F32)
    return grad_one, inn, out, taps


def solution(mesh):
    tokens = P("dp", "space", None, None)
    return jax.shard_map(
        shards,
        mesh=mesh,
        in_specs=(tokens, tokens, tokens, P(), P(), P(), tokens, P(), P(), P()),
        out_specs=(tokens, P("dp", None), P("dp", None), P()),
        check_vma=False,
    )
```

```python
import functools
import math

import jax
import jax.numpy as jnp
from jax import lax
from jax.experimental import pallas as pl
from jax.experimental.pallas import tpu as pltpu
from jax.sharding import PartitionSpec as P

MESH = pl.DeviceIdType.MESH
F32 = jnp.float32
BF16 = jnp.bfloat16
GELU_C = math.sqrt(2.0 / math.pi)
GELU_D = 0.044715 * GELU_C
NT = (((1,), (1,)), ((), ()))
NN = (((1,), (0,)), ((), ()))
TN = (((0,), (0,)), ((), ()))
LANES = 128
SHARES = (1, 1, 1)
STREAMS = len(SHARES)
LAGS = (0, 0, 1)
FREE, HELD, OPEN = 3, 5, 9
COMM = True
WEIGHTS = True
HALO = True


def dot(a, b, dims):
    return lax.dot_general(a, b, dims, preferred_element_type=F32)


def gelu_slope_parts(v):
    cube = GELU_D * (v * v)
    t = jnp.tanh(v * (cube + GELU_C))
    p = 1.0 + t
    act = (0.5 * v) * p
    slope = 0.5 * p + act * (1.0 - t) * (3.0 * cube + GELU_C)
    return act, slope


def bits_of(n):
    return (n - 1).bit_length()


def my_bit(index, bit):
    return (index // (1 << bit)) % 2


def flip(index, bit):
    return index + (1 << bit) * (1 - 2 * my_bit(index, bit))


def rolled(row, shift):
    if shift == 0:
        return row
    if shift == 1:
        return jnp.concatenate([row[-1:], row[:-1]], axis=0)
    return jnp.concatenate([row[1:], row[:1]], axis=0)


class Plan:
    def __init__(self, dp, space, hidden, width):
        self.dp, self.space = dp, space
        self.db, self.sb = bits_of(dp), bits_of(space)
        self.width = width
        rows = hidden // (dp * space)
        self.piece = next(q for q in (16, 8, rows) if rows % q == 0)
        self.chunks = rows // self.piece
        unit = width // sum(SHARES)
        self.lanes = [unit * share for share in SHARES]
        self.first = [unit * sum(SHARES[:n]) for n in range(STREAMS)]
        spaces = [("space", b) for b in range(self.sb)]
        rest = [("dp", b) for b in range(1, self.db)]
        self.orders = [spaces + rest, spaces[::-1] + rest, rest + spaces[::-1]]
        self.stages = self.sb + self.db - 1

    def labels(self):
        return [("dp", b) for b in reversed(range(self.db))] + [
            ("space", b) for b in reversed(range(self.sb))
        ]


def kernel(
    plan, shape, inv_batch,
    mixed_two, input_two, cotangent, w_in_two, w_out_two, kernel_two, mixed_one, w_in_one, w_out_one, kernel_one,
    out_ref, grads_ref, taps_out,
    raw_mixed, raw_input, raw_cot, raw_one, input_row,
    mixed, cot, early, w_in, w_out, w_late, act_t, pg_t, mix_acc, mix_row, grad_two, slope,
    halo_late, halo_early, taps, taps_in, gathered, *rest,
):
    count = (plan.stages + 1) * STREAMS
    term = rest[:STREAMS]
    stage_in = [rest[STREAMS + n : STREAMS + count : STREAMS] for n in range(STREAMS)]
    rest = rest[STREAMS + count :]
    (
        load_sem, weight_sem, late_sem, out_sem, own_sem,
        send_sem, recv_sem, gsend_sem, grecv_sem, hsend_sem, hrecv_sem, tsend_sem, trecv_sem,
    ) = rest
    rows, cols, width = shape
    tokens = mixed.shape[0]
    pad = tokens // rows
    T = act_t.shape[2]
    K = plan.chunks
    F = w_in.shape[0] * w_in.shape[2]
    dpi, spi = lax.axis_index("dp"), lax.axis_index("space")
    where = {"dp": dpi, "space": spi}
    labels = plan.labels()
    order = [0, rows - 1] + list(range(1, rows - 1))
    place = {r: n for n, r in enumerate(order)}

    loads = [
        pltpu.make_async_copy(src.at[0], dst, load_sem.at[n])
        for n, (src, dst) in enumerate(
            [(mixed_two, raw_mixed), (cotangent, raw_cot), (mixed_one, raw_one), (input_two, raw_input)]
        )
    ]

    def weight_load(k, which):
        src, dst = ((w_in_two, w_in), (w_out_two, w_out))[which]
        return pltpu.make_async_copy(src.at[:, k], dst.at[:, k], weight_sem.at[which, k])

    late_loads = [
        pltpu.make_async_copy(w_in_one, w_late, late_sem.at[0]),
        pltpu.make_async_copy(w_out_one, w_out, late_sem.at[1]),
    ]
    loads[0].start()
    weight_load(0, 0).start()
    loads[1].start()
    weight_load(0, 1).start()
    for k in range(1, K):
        weight_load(k, 0).start()
        weight_load(k, 1).start()
    loads[2].start()
    loads[3].start()
    late_loads[0].start()

    peers = [{"dp": flip(dpi, b)} for b in range(plan.db)]

    def across(offset):
        other = spi
        for b in range(plan.sb):
            if (offset >> b) & 1:
                other = flip(other, b)
        return other

    peers += [{"space": across(o)} for o in range(1, plan.space)]
    if COMM:
        barrier = pltpu.get_barrier_semaphore()
        for peer in peers:
            pl.semaphore_signal(barrier, inc=1, device_id=peer, device_id_type=MESH)

    zeros = jnp.zeros((16, width), BF16)
    for r in range(rows):
        mixed[pl.ds((r + 1) * pad - 16, 16)] = zeros
        cot[pl.ds((r + 1) * pad - 16, 16)] = zeros
        early[r, pl.ds(pad - 16, 16)] = zeros
        grad_two[r, pl.ds(pad - 16, 16)] = zeros
    mix_acc[...] = jnp.zeros_like(mix_acc)
    for halo in (halo_late, halo_early):
        pl.when(spi == 0)(lambda halo=halo: halo.__setitem__(0, jnp.zeros(halo.shape[1:], BF16)))
        pl.when(spi == plan.space - 1)(lambda halo=halo: halo.__setitem__(1, jnp.zeros(halo.shape[1:], BF16)))

    loads[0].wait()
    for r in range(rows):
        mixed[pl.ds(r * pad, cols)] = raw_mixed[:, r, :]
    loads[1].wait()
    for r in range(rows):
        cot[pl.ds(r * pad, cols)] = raw_cot[:, r, :]

    def half(done, now, value):
        index = []
        for label in labels:
            if label in done:
                index.append(my_bit(where[label[0]], label[1]))
            elif label == now:
                index.append(value)
            else:
                index.append(slice(None))
        return tuple(index)

    def exchange(k, stage, stream):
        now = ("dp", 0) if stage == 0 else plan.orders[stream][stage - 1]
        done = ([("dp", 0)] + plan.orders[stream])[:stage]
        mine = my_bit(where[now[0]], now[1])
        kept = (k, slice(None)) + half(done, now, mine)
        came = stage_in[stream][stage].at[k]
        copy = pltpu.make_async_remote_copy(
            src_ref=term[stream].at[(k, slice(None)) + half(done, now, 1 - mine)],
            dst_ref=came,
            send_sem=send_sem.at[k, stage, stream],
            recv_sem=recv_sem.at[k, stage, stream],
            device_id={now[0]: flip(where[now[0]], now[1])},
            device_id_type=MESH,
        )
        return copy, kept, came

    def gather(k, bit):
        pieces = gathered.at[k, pl.ds(spi // (1 << bit) * (1 << bit), 1 << bit)]
        return pltpu.make_async_remote_copy(
            src_ref=pieces,
            dst_ref=pieces,
            send_sem=gsend_sem.at[k, bit],
            recv_sem=grecv_sem.at[k, bit],
            device_id={"space": flip(spi, bit)},
            device_id_type=MESH,
        )

    def own(k):
        return pltpu.make_async_copy(gathered.at[k], grads_ref.at[k], own_sem.at[k])

    def start(k, stage):
        if not (COMM and WEIGHTS):
            return
        for stream in range(STREAMS):
            exchange(k, stage, stream)[0].start()

    def finish(k, stage, stream):
        if not (COMM and WEIGHTS):
            return
        copy, kept, came = exchange(k, stage, stream)
        copy.wait()
        if stage == 0:
            for a in range(2):
                index = (k, a) + kept[2:]
                total = term[stream][index].astype(F32) + came[a].astype(F32)
                term[stream][index] = total.astype(BF16)
        else:
            total = (term[stream][kept].astype(F32) + came[...].astype(F32)).astype(BF16)
            if stage == plan.stages:
                gathered[k, spi, :, :, pl.ds(plan.first[stream], plan.lanes[stream])] = total
            else:
                term[stream][kept] = total
        if stage < plan.stages:
            exchange(k, stage + 1, stream)[0].start()

    def spread_out(k, bit):
        if not (COMM and WEIGHTS):
            return
        if bit >= 0:
            gather(k, bit).wait()
        if bit + 1 < plan.sb:
            gather(k, bit + 1).start()
        else:
            own(k).start()

    def tick(i):
        for stage in reversed(range(plan.stages + 1)):
            for stream in range(STREAMS):
                back = i - 1 - stage - (LAGS[stream] if stage > 0 else 0)
                if stage + 1 + (LAGS[stream] if stage > 0 else 0) < K:
                    pl.when(back >= 0)(functools.partial(finish, back, stage, stream))

    left = {}
    for k in range(K):
        for stream in range(STREAMS):
            done = K - 1 - k
            later = max(0, min(plan.stages, done - 1 - LAGS[stream]))
            left[k, stream] = [min(done, 1) + later, -1]
        left[k, STREAMS] = [plan.stages + 1, None]

    def axis_of(stage, stream):
        if stream == STREAMS:
            return ("space", stage - plan.stages - 1)
        return ("dp", 0) if stage == 0 else plan.orders[stream][stage - 1]

    def slot(j):
        for k in range(K):
            for stream in range(STREAMS + 1):
                stage, began = left[k, stream]
                if stream == STREAMS:
                    if began is None and all(left[k, n][0] > plan.stages for n in range(STREAMS)):
                        spread_out(k, -1)
                        left[k, stream][1] = j
                        continue
                    if began is None or stage > plan.stages + plan.sb:
                        continue
                elif stage > plan.stages:
                    continue
                if began >= j:
                    continue
                axis, bit = axis_of(stage, stream)
                if axis == "space" and j < (FREE if began < HELD else OPEN):
                    continue
                if stream == STREAMS and j < (OPEN if bit > 0 or began >= HELD else HELD):
                    continue
                if stream == STREAMS:
                    spread_out(k, stage - plan.stages - 1)
                else:
                    finish(k, stage, stream)
                left[k, stream] = [stage + 1, j]

    def late_chunk(k, carry):
        weight_load(k, 0).wait()
        weight_load(k, 1).wait()

        wi = w_in[:, k].reshape(F, width)
        wo = w_out[:, k].reshape(F, width)

        def tile(t, c):
            v = dot(wi, mixed[pl.ds(t * T, T)], NT)
            h = dot(wo, cot[pl.ds(t * T, T)], NT)
            act, grad = gelu_slope_parts(v)
            act_t[t] = act.astype(BF16)
            pg_t[t] = (h * grad).astype(BF16)
            return c

        for t in range(tokens // T):
            tile(t, 0)
        if COMM:
            pl.when(k == 0)(lambda: pl.semaphore_wait(barrier, len(peers)))
        for t in range(tokens // T):
            mix_acc[pl.ds(t * T, T)] += dot(pg_t[t], wi, TN)

        @pl.when(k == K - 1)
        def _():
            for r in range(rows):
                mix_row[r] = mix_acc[pl.ds(r * pad, cols)].astype(BF16)
            halo_start(mix_row, halo_late, 0)

        tick(k)

        def put(a, value):
            value = (value * inv_batch).astype(BF16)
            for s in range(STREAMS):
                part = value[:, plan.first[s] : plan.first[s] + plan.lanes[s]]
                term[s][k, a] = part.reshape(term[s].shape[2:])

        def against(lhs, rhs):
            total = dot(lhs[0], rhs[pl.ds(0, T)], NN)
            for t in range(1, tokens // T):
                total = total + dot(lhs[t], rhs[pl.ds(t * T, T)], NN)
            return total

        put(0, against(act_t, cot))
        put(1, against(pg_t, mixed))
        start(k, 0)
        return carry

    def halo_copy(rows_ref, halo, side, which):
        src = rows_ref.at[0 if side == 0 else rows - 1]
        return pltpu.make_async_remote_copy(
            src_ref=src,
            dst_ref=halo.at[1 - side],
            send_sem=hsend_sem.at[which, side],
            recv_sem=hrecv_sem.at[which, 1 - side],
            device_id={"space": spi - 1 if side == 0 else spi + 1},
            device_id_type=MESH,
        )

    def halo_do(rows_ref, halo, which, act):
        if not (COMM and HALO):
            return
        pl.when(spi > 0)(lambda: act(halo_copy(rows_ref, halo, 0, which), 0))
        pl.when(spi < plan.space - 1)(lambda: act(halo_copy(rows_ref, halo, 1, which), 1))

    def halo_start(rows_ref, halo, which):
        halo_do(rows_ref, halo, which, lambda copy, side: copy.start())

    def halo_wait(rows_ref, halo, which):
        def wait(copy, side):
            copy.wait_send()
            pltpu.make_async_remote_copy(
                src_ref=rows_ref.at[0],
                dst_ref=halo.at[side],
                send_sem=hsend_sem.at[which, side],
                recv_sem=hrecv_sem.at[which, side],
                device_id={"space": spi - 1 if side == 0 else spi + 1},
                device_id_type=MESH,
            ).wait_recv()

        halo_do(rows_ref, halo, which, wait)

    lax.fori_loop(0, K, late_chunk, 0)
    late_loads[1].start()
    slots = iter(range(64))

    def next_tick():
        slot(next(slots))

    def conv(wanted, halo, rows_ref, kernel_ref, base, store, with_taps):
        def block(c, carry):
            lanes = pl.ds(pl.multiple_of(c * LANES, LANES), LANES)
            weights = kernel_ref[:, lanes].astype(F32)
            windows = {}
            sums = [None] * 9
            for i in wanted:
                total = base(i, lanes).astype(F32)
                held = input_row[i, :, lanes].astype(F32) if with_taps else None
                for lat in range(3):
                    p = i + 2 - lat
                    if p not in windows:
                        if p == 0:
                            row = halo[0, :, lanes]
                        elif p == rows + 1:
                            row = halo[1, :, lanes]
                        else:
                            row = rows_ref[p - 1, :, lanes]
                        windows[p] = [rolled(row.astype(F32), b - 1) for b in range(3)]
                    for lon in range(3):
                        tap = 3 * lat + lon
                        total = total + weights[tap : tap + 1] * windows[p][lon]
                        if with_taps:
                            part = jnp.sum(held * windows[p][lon], axis=0, keepdims=True)
                            sums[tap] = part if sums[tap] is None else sums[tap] + part
                store(i, lanes, total.astype(BF16))
            if with_taps:
                for tap in range(9):
                    taps[tap : tap + 1, lanes] += sums[tap]
            return carry

        lax.fori_loop(0, width // LANES, block, 0)

    loads[2].wait()
    for r in range(rows):
        early[place[r], pl.ds(0, cols)] = raw_one[:, r, :]
    late_loads[0].wait()
    hidden = w_late.shape[0]
    E = slope.shape[2]
    steps = hidden // E

    def early_slope(n, carry):
        w = w_late[pl.ds(pl.multiple_of(n * E, E), E)]
        for r in range(0, rows, 2):
            v = dot(early[pl.ds(r, 2)].reshape(2 * pad, width), w, NT)
            slope[n, pl.ds(r * pad, 2 * pad)] = gelu_slope_parts(v)[1].astype(BF16)
        return carry

    lax.fori_loop(0, steps // 2, early_slope, 0)
    next_tick()
    lax.fori_loop(steps // 2, steps, early_slope, 0)
    next_tick()
    loads[3].wait()
    for r in range(rows):
        input_row[r] = raw_input[:, r, :]
    taps[...] = jnp.zeros_like(taps)

    def late_base(i, lanes):
        return cot[pl.ds(i * pad, cols), lanes]

    def late_store(i, lanes, value):
        grad_two[place[i], pl.ds(0, cols), lanes] = value

    conv(range(1, rows - 1), halo_late, mix_row, kernel_two, late_base, late_store, True)
    next_tick()
    halo_wait(mix_row, halo_late, 0)
    conv([0, rows - 1], halo_late, mix_row, kernel_two, late_base, late_store, True)
    taps[...] = taps[...] * inv_batch

    moves = [("space", b) for b in range(plan.sb)] + [("dp", b) for b in range(plan.db)]

    def taps_copy(n):
        axis, bit = moves[n]
        return pltpu.make_async_remote_copy(
            src_ref=taps,
            dst_ref=taps_in.at[n],
            send_sem=tsend_sem.at[n],
            recv_sem=trecv_sem.at[n],
            device_id={axis: flip(where[axis], bit)},
            device_id_type=MESH,
        )

    def taps_step(n):
        if not (COMM and HALO):
            return
        if 0 < n <= len(moves):
            taps_copy(n - 1).wait()
            taps[...] += taps_in[n - 1]
        if n < len(moves):
            taps_copy(n).start()

    taps_step(0)
    next_tick()
    steps_taps = iter(range(1, len(moves) + 1))

    def next_taps():
        n = next(steps_taps, None)
        if n is not None:
            taps_step(n)

    late_loads[1].wait()
    w_out_flat = w_out.reshape(hidden, width)

    def early_group(first, count):
        span = count * pad
        lo = first * pad

        def chunk(n, carry):
            w_o = w_out_flat[pl.ds(pl.multiple_of(n * E, E), E)]
            w_i = w_late[pl.ds(pl.multiple_of(n * E, E), E)]
            h = dot(grad_two[pl.ds(first, count)].reshape(span, width), w_o, NT)
            s = slope[n, pl.ds(lo, span)].astype(F32)
            g = (h * s).astype(BF16)
            back = dot(g, w_i, NN)
            for r in range(count):
                mix_acc[pl.ds((first + r) * pad, pad)] += back[r * pad : (r + 1) * pad]
            return carry

        for r in range(count):
            mix_acc[pl.ds((first + r) * pad, pad)] = jnp.zeros((pad, width), F32)
        lax.fori_loop(0, steps // 2, chunk, 0)
        next_taps()
        next_tick()
        lax.fori_loop(steps // 2, steps, chunk, 0)
        for r in range(count):
            mix_row[order[first + r]] = mix_acc[pl.ds((first + r) * pad, cols)].astype(BF16)

    early_group(0, 2)
    halo_start(mix_row, halo_early, 1)
    next_taps()
    next_tick()
    early_group(2, rows - 2)
    next_taps()
    next_tick()

    def early_base(i, lanes):
        return grad_two[place[i], pl.ds(0, cols), lanes]

    def early_store(i, lanes, value):
        input_row[i, :, lanes] = value

    def out_copy(i):
        return pltpu.make_async_copy(input_row.at[i], out_ref.at[0, i], out_sem.at[i])

    conv(range(1, rows - 1), halo_early, mix_row, kernel_one, early_base, early_store, False)
    for i in range(1, rows - 1):
        out_copy(i).start()
    next_tick()
    halo_wait(mix_row, halo_early, 1)
    next_tick()
    conv([0, rows - 1], halo_early, mix_row, kernel_one, early_base, early_store, False)
    out_copy(0).start()
    out_copy(rows - 1).start()
    for _ in range(plan.stages + plan.sb + 1):
        next_tick()
    for _ in moves:
        next_taps()
    taps_out[...] = taps[...]
    if COMM and WEIGHTS:
        for k in range(K):
            own(k).wait()
    for i in range(rows):
        out_copy(i).wait()


def whole_call(plan, inv_batch, args):
    mixed_two, input_two, cotangent, w_in_two, w_out_two, kernel_two, mixed_one, w_in_one, w_out_one, kernel_one = args
    _, rows, cols, width = mixed_two.shape
    hidden = w_in_two.shape[0]
    pad = -(-cols // 16) * 16
    K, dp, space, Q = plan.chunks, plan.dp, plan.space, plan.piece
    R = space * Q
    F = dp * R
    E = 512
    tokens = rows * pad
    T = next(t for t in (256, pad) if tokens % t == 0)
    w_in_two = w_in_two.reshape(dp, K, R, width)
    w_out_two = w_out_two.reshape(dp, K, R, width)
    w_out_one = w_out_one.reshape(dp, K, R, width)

    def turned(x):
        return jnp.transpose(x, (0, 2, 1, 3))

    anywhere = pl.BlockSpec(memory_space=pl.ANY)
    vmem = pl.BlockSpec(memory_space=pltpu.VMEM)
    bits = plan.db + plan.sb
    piece_shapes = [
        pltpu.VMEM((K, 2) + (2,) * (bits - step) + (Q, lanes), BF16)
        for step in range(bits + 1)
        for lanes in plan.lanes
    ]
    token = pltpu.VMEM((rows, pad, width), BF16)
    flat = pltpu.VMEM((tokens, width), BF16)
    lying = pltpu.VMEM((cols, rows, width), BF16)
    raw = pltpu.VMEM((rows, cols, width), BF16)
    taps = kernel_two.shape[0]
    moves = plan.db + plan.sb
    dma = pltpu.SemaphoreType.DMA
    scratch = [
        lying, lying, lying, lying, raw,
        flat, flat, token,
        pltpu.VMEM((dp, K, R, width), BF16),
        pltpu.VMEM((dp, K, R, width), BF16),
        pltpu.VMEM((hidden, width), BF16),
        pltpu.VMEM((tokens // T, F, T), BF16),
        pltpu.VMEM((tokens // T, F, T), BF16),
        pltpu.VMEM((tokens, width), F32),
        raw,
        token,
        pltpu.VMEM((hidden // E, rows * pad, E), BF16),
        pltpu.VMEM((2, cols, width), BF16),
        pltpu.VMEM((2, cols, width), BF16),
        pltpu.VMEM((taps, width), F32),
        pltpu.VMEM((moves, taps, width), F32),
        pltpu.VMEM((K, space, 2, Q, width), BF16),
        *piece_shapes,
        dma((4,)), dma((2, K)), dma((2,)), dma((rows,)), dma((K,)),
        dma((K, plan.stages + 1, STREAMS)), dma((K, plan.stages + 1, STREAMS)),
        dma((K, plan.sb)), dma((K, plan.sb)),
        dma((2, 2)), dma((2, 2)), dma((moves,)), dma((moves,)),
    ]
    return pl.pallas_call(
        functools.partial(kernel, plan, (rows, cols, width), inv_batch),
        in_specs=[anywhere] * 5 + [vmem] + [anywhere] * 3 + [vmem],
        out_specs=[anywhere, anywhere, vmem],
        out_shape=[
            jax.ShapeDtypeStruct(mixed_two.shape, BF16),
            jax.ShapeDtypeStruct((K, space, 2, Q, width), BF16),
            jax.ShapeDtypeStruct((taps, width), F32),
        ],
        scratch_shapes=scratch,
        compiler_params=pltpu.CompilerParams(
            collective_id=0 if COMM else None, has_side_effects=True, vmem_limit_bytes=67_043_328
        ),
    )(
        turned(mixed_two), turned(input_two), turned(cotangent), w_in_two, w_out_two, kernel_two,
        turned(mixed_one), w_in_one, w_out_one, kernel_one,
    )


def shards(*args):
    dp, space = lax.axis_size("dp"), lax.axis_size("space")
    samples, width, hidden = args[0].shape[0], args[0].shape[3], args[3].shape[0]
    plan = Plan(dp, space, hidden, width)
    grad_one, grads, taps = whole_call(plan, 1.0 / (samples * dp), args)
    out = grads[:, :, 0].reshape(-1, width).astype(F32)
    inn = grads[:, :, 1].reshape(-1, width).astype(F32)
    return grad_one, inn, out, taps


def solution(mesh):
    tokens = P("dp", "space", None, None)
    return jax.shard_map(
        shards,
        mesh=mesh,
        in_specs=(tokens, tokens, tokens, P(), P(), P(), tokens, P(), P(), P()),
        out_specs=(tokens, P("dp", None), P("dp", None), P()),
        check_vma=False,
    )
```

```python
import functools
import math

import jax
import jax.numpy as jnp
from jax import lax
from jax.experimental import pallas as pl
from jax.experimental.pallas import tpu as pltpu
from jax.sharding import PartitionSpec as P

MESH = pl.DeviceIdType.MESH
F32 = jnp.float32
BF16 = jnp.bfloat16
GELU_C = math.sqrt(2.0 / math.pi)
GELU_D = 0.044715 * GELU_C
NT = (((1,), (1,)), ((), ()))
NN = (((1,), (0,)), ((), ()))
TN = (((0,), (0,)), ((), ()))
LANES = 128
SHARES = (1, 1, 1)
STREAMS = len(SHARES)
LAGS = (0, 0, 1)
FREE, HELD, OPEN, END = 2, 4, 7, 9
COMM = True
WEIGHTS = True
HALO = True


def dot(a, b, dims):
    return lax.dot_general(a, b, dims, preferred_element_type=F32)


def gelu_slope_parts(v):
    cube = GELU_D * (v * v)
    t = jnp.tanh(v * (cube + GELU_C))
    p = 1.0 + t
    act = (0.5 * v) * p
    slope = 0.5 * p + act * (1.0 - t) * (3.0 * cube + GELU_C)
    return act, slope


def bits_of(n):
    return (n - 1).bit_length()


def my_bit(index, bit):
    return (index // (1 << bit)) % 2


def flip(index, bit):
    return index + (1 << bit) * (1 - 2 * my_bit(index, bit))


def rolled(row, shift):
    if shift == 0:
        return row
    if shift == 1:
        return jnp.concatenate([row[-1:], row[:-1]], axis=0)
    return jnp.concatenate([row[1:], row[:1]], axis=0)


class Plan:
    def __init__(self, dp, space, hidden, width):
        self.dp, self.space = dp, space
        self.db, self.sb = bits_of(dp), bits_of(space)
        self.width = width
        rows = hidden // (dp * space)
        self.piece = next(q for q in (16, 8, rows) if rows % q == 0)
        self.chunks = rows // self.piece
        unit = width // sum(SHARES)
        self.lanes = [unit * share for share in SHARES]
        self.first = [unit * sum(SHARES[:n]) for n in range(STREAMS)]
        spaces = [("space", b) for b in range(self.sb)]
        rest = [("dp", b) for b in range(1, self.db)]
        self.orders = [spaces + rest, spaces[::-1] + rest, rest + spaces[::-1]]
        self.stages = self.sb + self.db - 1

    def labels(self):
        return [("dp", b) for b in reversed(range(self.db))] + [
            ("space", b) for b in reversed(range(self.sb))
        ]


def kernel(
    plan, shape, inv_batch,
    mixed_two, input_two, cotangent, w_in_two, w_out_two, kernel_two, mixed_one, w_in_one, w_out_one, kernel_one,
    out_ref, grads_ref, taps_out,
    raw_mixed, raw_input, raw_cot, raw_one, input_row,
    mixed, cot, early, w_in, w_out, w_late, act_t, pg_t, mix_acc, mix_row, grad_two, slope,
    halo_late, halo_early, taps, taps_in, gathered, *rest,
):
    count = (plan.stages + 1) * STREAMS
    term = rest[:STREAMS]
    stage_in = [rest[STREAMS + n : STREAMS + count : STREAMS] for n in range(STREAMS)]
    rest = rest[STREAMS + count :]
    (
        load_sem, weight_sem, late_sem, out_sem, own_sem,
        send_sem, recv_sem, gsend_sem, grecv_sem, hsend_sem, hrecv_sem, tsend_sem, trecv_sem,
    ) = rest
    rows, cols, width = shape
    tokens = mixed.shape[0]
    pad = tokens // rows
    T = act_t.shape[2]
    K = plan.chunks
    F = w_in.shape[0] * w_in.shape[2]
    dpi, spi = lax.axis_index("dp"), lax.axis_index("space")
    where = {"dp": dpi, "space": spi}
    labels = plan.labels()
    order = [0, rows - 1] + list(range(1, rows - 1))
    place = {r: n for n, r in enumerate(order)}

    loads = [
        pltpu.make_async_copy(src.at[0], dst, load_sem.at[n])
        for n, (src, dst) in enumerate(
            [(mixed_two, raw_mixed), (cotangent, raw_cot), (mixed_one, raw_one), (input_two, raw_input)]
        )
    ]

    def weight_load(k, which):
        src, dst = ((w_in_two, w_in), (w_out_two, w_out))[which]
        return pltpu.make_async_copy(src.at[:, k], dst.at[:, k], weight_sem.at[which, k])

    late_loads = [
        pltpu.make_async_copy(w_in_one, w_late, late_sem.at[0]),
        pltpu.make_async_copy(w_out_one, w_out, late_sem.at[1]),
    ]
    loads[0].start()
    weight_load(0, 0).start()
    loads[1].start()
    weight_load(0, 1).start()
    for k in range(1, K):
        weight_load(k, 0).start()
        weight_load(k, 1).start()
    loads[2].start()
    loads[3].start()
    late_loads[0].start()

    peers = [{"dp": flip(dpi, b)} for b in range(plan.db)]

    def across(offset):
        other = spi
        for b in range(plan.sb):
            if (offset >> b) & 1:
                other = flip(other, b)
        return other

    peers += [{"space": across(o)} for o in range(1, plan.space)]
    if COMM:
        barrier = pltpu.get_barrier_semaphore()
        for peer in peers:
            pl.semaphore_signal(barrier, inc=1, device_id=peer, device_id_type=MESH)

    zeros = jnp.zeros((16, width), BF16)
    for r in range(rows):
        mixed[pl.ds((r + 1) * pad - 16, 16)] = zeros
        cot[pl.ds((r + 1) * pad - 16, 16)] = zeros
        early[r, pl.ds(pad - 16, 16)] = zeros
        grad_two[r, pl.ds(pad - 16, 16)] = zeros
    mix_acc[...] = jnp.zeros_like(mix_acc)
    for halo in (halo_late, halo_early):
        pl.when(spi == 0)(lambda halo=halo: halo.__setitem__(0, jnp.zeros(halo.shape[1:], BF16)))
        pl.when(spi == plan.space - 1)(lambda halo=halo: halo.__setitem__(1, jnp.zeros(halo.shape[1:], BF16)))

    loads[0].wait()
    for r in range(rows):
        mixed[pl.ds(r * pad, cols)] = raw_mixed[:, r, :]
    loads[1].wait()
    for r in range(rows):
        cot[pl.ds(r * pad, cols)] = raw_cot[:, r, :]

    def half(done, now, value):
        index = []
        for label in labels:
            if label in done:
                index.append(my_bit(where[label[0]], label[1]))
            elif label == now:
                index.append(value)
            else:
                index.append(slice(None))
        return tuple(index)

    def exchange(k, stage, stream):
        now = ("dp", 0) if stage == 0 else plan.orders[stream][stage - 1]
        done = ([("dp", 0)] + plan.orders[stream])[:stage]
        mine = my_bit(where[now[0]], now[1])
        kept = (k, slice(None)) + half(done, now, mine)
        came = stage_in[stream][stage].at[k]
        copy = pltpu.make_async_remote_copy(
            src_ref=term[stream].at[(k, slice(None)) + half(done, now, 1 - mine)],
            dst_ref=came,
            send_sem=send_sem.at[k, stage, stream],
            recv_sem=recv_sem.at[k, stage, stream],
            device_id={now[0]: flip(where[now[0]], now[1])},
            device_id_type=MESH,
        )
        return copy, kept, came

    def gather(k, bit):
        pieces = gathered.at[k, pl.ds(spi // (1 << bit) * (1 << bit), 1 << bit)]
        return pltpu.make_async_remote_copy(
            src_ref=pieces,
            dst_ref=pieces,
            send_sem=gsend_sem.at[k, bit],
            recv_sem=grecv_sem.at[k, bit],
            device_id={"space": flip(spi, bit)},
            device_id_type=MESH,
        )

    def own(k):
        return pltpu.make_async_copy(gathered.at[k], grads_ref.at[k], own_sem.at[k])

    def start(k, stage):
        if not (COMM and WEIGHTS):
            return
        for stream in range(STREAMS):
            exchange(k, stage, stream)[0].start()

    def finish(k, stage, stream):
        if not (COMM and WEIGHTS):
            return
        copy, kept, came = exchange(k, stage, stream)
        copy.wait()
        if stage == 0:
            for a in range(2):
                index = (k, a) + kept[2:]
                total = term[stream][index].astype(F32) + came[a].astype(F32)
                term[stream][index] = total.astype(BF16)
        else:
            total = (term[stream][kept].astype(F32) + came[...].astype(F32)).astype(BF16)
            if stage == plan.stages:
                gathered[k, spi, :, :, pl.ds(plan.first[stream], plan.lanes[stream])] = total
            else:
                term[stream][kept] = total
        if stage < plan.stages:
            exchange(k, stage + 1, stream)[0].start()

    def spread_out(k, bit):
        if not (COMM and WEIGHTS):
            return
        if bit >= 0:
            gather(k, bit).wait()
        if bit + 1 < plan.sb:
            gather(k, bit + 1).start()
        else:
            own(k).start()

    def tick(i):
        for stage in reversed(range(plan.stages + 1)):
            for stream in range(STREAMS):
                back = i - 1 - stage - (LAGS[stream] if stage > 0 else 0)
                if stage + 1 + (LAGS[stream] if stage > 0 else 0) < K:
                    pl.when(back >= 0)(functools.partial(finish, back, stage, stream))

    left = {}
    for k in range(K):
        for stream in range(STREAMS):
            done = K - 1 - k
            later = max(0, min(plan.stages, done - 1 - LAGS[stream]))
            left[k, stream] = [min(done, 1) + later, -1]
        left[k, STREAMS] = [plan.stages + 1, None]

    def axis_of(stage, stream):
        if stream == STREAMS:
            return ("space", stage - plan.stages - 1)
        return ("dp", 0) if stage == 0 else plan.orders[stream][stage - 1]

    def slot(j):
        for k in range(K):
            for stream in range(STREAMS + 1):
                stage, began = left[k, stream]
                if stream == STREAMS:
                    if began is None and all(left[k, n][0] > plan.stages for n in range(STREAMS)):
                        spread_out(k, -1)
                        left[k, stream][1] = j
                        continue
                    if began is None or stage > plan.stages + plan.sb:
                        continue
                elif stage > plan.stages:
                    continue
                if began >= j:
                    continue
                if 0 <= began and j - began < (2 if k < K - 1 and j < 3 and stream < STREAMS else 1):
                    continue
                axis, bit = axis_of(stage, stream)
                if axis == "space" and j < (FREE if began < HELD else OPEN):
                    continue
                if stream == STREAMS and j < (END if bit > 0 else OPEN if began >= HELD else HELD):
                    continue
                if stream == STREAMS:
                    spread_out(k, stage - plan.stages - 1)
                else:
                    finish(k, stage, stream)
                left[k, stream] = [stage + 1, j]

    def late_chunk(k, carry):
        weight_load(k, 0).wait()
        weight_load(k, 1).wait()

        wi = w_in[:, k].reshape(F, width)
        wo = w_out[:, k].reshape(F, width)

        def tile(t, c):
            v = dot(wi, mixed[pl.ds(t * T, T)], NT)
            h = dot(wo, cot[pl.ds(t * T, T)], NT)
            act, grad = gelu_slope_parts(v)
            act_t[t] = act.astype(BF16)
            pg_t[t] = (h * grad).astype(BF16)
            return c

        for t in range(tokens // T):
            tile(t, 0)
        if COMM:
            pl.when(k == 0)(lambda: pl.semaphore_wait(barrier, len(peers)))
        for t in range(tokens // T):
            mix_acc[pl.ds(t * T, T)] += dot(pg_t[t], wi, TN)

        @pl.when(k == K - 1)
        def _():
            for r in range(rows):
                mix_row[r] = mix_acc[pl.ds(r * pad, cols)].astype(BF16)
            halo_start(mix_row, halo_late, 0)

        tick(k)

        def put(a, value):
            value = (value * inv_batch).astype(BF16)
            for s in range(STREAMS):
                part = value[:, plan.first[s] : plan.first[s] + plan.lanes[s]]
                term[s][k, a] = part.reshape(term[s].shape[2:])

        def against(lhs, rhs):
            total = dot(lhs[0], rhs[pl.ds(0, T)], NN)
            for t in range(1, tokens // T):
                total = total + dot(lhs[t], rhs[pl.ds(t * T, T)], NN)
            return total

        put(0, against(act_t, cot))
        put(1, against(pg_t, mixed))
        start(k, 0)
        return carry

    def halo_copy(rows_ref, halo, side, which):
        src = rows_ref.at[0 if side == 0 else rows - 1]
        return pltpu.make_async_remote_copy(
            src_ref=src,
            dst_ref=halo.at[1 - side],
            send_sem=hsend_sem.at[which, side],
            recv_sem=hrecv_sem.at[which, 1 - side],
            device_id={"space": spi - 1 if side == 0 else spi + 1},
            device_id_type=MESH,
        )

    def halo_do(rows_ref, halo, which, act):
        if not (COMM and HALO):
            return
        pl.when(spi > 0)(lambda: act(halo_copy(rows_ref, halo, 0, which), 0))
        pl.when(spi < plan.space - 1)(lambda: act(halo_copy(rows_ref, halo, 1, which), 1))

    def halo_start(rows_ref, halo, which):
        halo_do(rows_ref, halo, which, lambda copy, side: copy.start())

    def halo_wait(rows_ref, halo, which):
        def wait(copy, side):
            copy.wait_send()
            pltpu.make_async_remote_copy(
                src_ref=rows_ref.at[0],
                dst_ref=halo.at[side],
                send_sem=hsend_sem.at[which, side],
                recv_sem=hrecv_sem.at[which, side],
                device_id={"space": spi - 1 if side == 0 else spi + 1},
                device_id_type=MESH,
            ).wait_recv()

        halo_do(rows_ref, halo, which, wait)

    lax.fori_loop(0, K, late_chunk, 0)
    late_loads[1].start()
    slots = iter(range(64))

    def next_tick():
        slot(next(slots))

    def conv(wanted, halo, rows_ref, kernel_ref, base, store, with_taps):
        def block(c, carry):
            lanes = pl.ds(pl.multiple_of(c * LANES, LANES), LANES)
            weights = kernel_ref[:, lanes].astype(F32)
            windows = {}
            sums = [None] * 9
            for i in wanted:
                total = base(i, lanes).astype(F32)
                held = input_row[i, :, lanes].astype(F32) if with_taps else None
                for lat in range(3):
                    p = i + 2 - lat
                    if p not in windows:
                        if p == 0:
                            row = halo[0, :, lanes]
                        elif p == rows + 1:
                            row = halo[1, :, lanes]
                        else:
                            row = rows_ref[p - 1, :, lanes]
                        windows[p] = [rolled(row.astype(F32), b - 1) for b in range(3)]
                    for lon in range(3):
                        tap = 3 * lat + lon
                        total = total + weights[tap : tap + 1] * windows[p][lon]
                        if with_taps:
                            part = jnp.sum(held * windows[p][lon], axis=0, keepdims=True)
                            sums[tap] = part if sums[tap] is None else sums[tap] + part
                store(i, lanes, total.astype(BF16))
            if with_taps:
                for tap in range(9):
                    taps[tap : tap + 1, lanes] += sums[tap]
            return carry

        lax.fori_loop(0, width // LANES, block, 0)

    loads[2].wait()
    for r in range(rows):
        early[place[r], pl.ds(0, cols)] = raw_one[:, r, :]
    late_loads[0].wait()
    hidden = w_late.shape[0]
    E = slope.shape[2]
    steps = hidden // E

    def early_slope(first, count):
        def step(n, carry):
            w = w_late[pl.ds(pl.multiple_of(n * E, E), E)]
            v = dot(early[pl.ds(first, count)].reshape(count * pad, width), w, NT)
            slope[n, pl.ds(first * pad, count * pad)] = gelu_slope_parts(v)[1].astype(BF16)
            return carry

        lax.fori_loop(0, steps, step, 0)

    early_slope(0, 2)
    next_tick()
    loads[3].wait()
    for r in range(rows):
        input_row[r] = raw_input[:, r, :]
    taps[...] = jnp.zeros_like(taps)

    def late_base(i, lanes):
        return cot[pl.ds(i * pad, cols), lanes]

    def late_store(i, lanes, value):
        grad_two[place[i], pl.ds(0, cols), lanes] = value

    conv(range(1, rows - 1), halo_late, mix_row, kernel_two, late_base, late_store, True)
    next_tick()
    halo_wait(mix_row, halo_late, 0)
    conv([0, rows - 1], halo_late, mix_row, kernel_two, late_base, late_store, True)
    taps[...] = taps[...] * inv_batch

    moves = [("space", b) for b in range(plan.sb)] + [("dp", b) for b in range(plan.db)]

    def taps_copy(n):
        axis, bit = moves[n]
        return pltpu.make_async_remote_copy(
            src_ref=taps,
            dst_ref=taps_in.at[n],
            send_sem=tsend_sem.at[n],
            recv_sem=trecv_sem.at[n],
            device_id={axis: flip(where[axis], bit)},
            device_id_type=MESH,
        )

    def taps_step(n):
        if not (COMM and HALO):
            return
        if 0 < n <= len(moves):
            taps_copy(n - 1).wait()
            taps[...] += taps_in[n - 1]
        if n < len(moves):
            taps_copy(n).start()

    taps_step(0)
    next_tick()
    steps_taps = iter(range(1, len(moves) + 1))

    def next_taps():
        n = next(steps_taps, None)
        if n is not None:
            taps_step(n)

    late_loads[1].wait()
    w_out_flat = w_out.reshape(hidden, width)

    def early_group(first, count):
        span = count * pad
        lo = first * pad

        def chunk(n, carry):
            w_o = w_out_flat[pl.ds(pl.multiple_of(n * E, E), E)]
            w_i = w_late[pl.ds(pl.multiple_of(n * E, E), E)]
            h = dot(grad_two[pl.ds(first, count)].reshape(span, width), w_o, NT)
            s = slope[n, pl.ds(lo, span)].astype(F32)
            g = (h * s).astype(BF16)
            back = dot(g, w_i, NN)
            for r in range(count):
                mix_acc[pl.ds((first + r) * pad, pad)] += back[r * pad : (r + 1) * pad]
            return carry

        for r in range(count):
            mix_acc[pl.ds((first + r) * pad, pad)] = jnp.zeros((pad, width), F32)
        lax.fori_loop(0, steps // 2, chunk, 0)
        next_taps()
        next_tick()
        lax.fori_loop(steps // 2, steps, chunk, 0)
        for r in range(count):
            mix_row[order[first + r]] = mix_acc[pl.ds((first + r) * pad, cols)].astype(BF16)

    early_group(0, 2)
    halo_start(mix_row, halo_early, 1)
    next_taps()
    next_tick()
    early_slope(2, rows - 2)
    next_taps()
    next_tick()
    early_group(2, rows - 2)
    next_tick()

    def early_base(i, lanes):
        return grad_two[place[i], pl.ds(0, cols), lanes]

    def early_store(i, lanes, value):
        input_row[i, :, lanes] = value

    def out_copy(i):
        return pltpu.make_async_copy(input_row.at[i], out_ref.at[0, i], out_sem.at[i])

    conv(range(1, rows - 1), halo_early, mix_row, kernel_one, early_base, early_store, False)
    for i in range(1, rows - 1):
        out_copy(i).start()
    next_tick()
    halo_wait(mix_row, halo_early, 1)
    conv([0, rows - 1], halo_early, mix_row, kernel_one, early_base, early_store, False)
    out_copy(0).start()
    out_copy(rows - 1).start()
    for _ in range(plan.stages + plan.sb + 1):
        next_tick()
    assert all(stage == plan.stages + 1 + (plan.sb if n == STREAMS else 0) for (_, n), (stage, _) in left.items())
    for _ in moves:
        next_taps()
    taps_out[...] = taps[...]
    if COMM and WEIGHTS:
        for k in range(K):
            own(k).wait()
    for i in range(rows):
        out_copy(i).wait()


def whole_call(plan, inv_batch, args):
    mixed_two, input_two, cotangent, w_in_two, w_out_two, kernel_two, mixed_one, w_in_one, w_out_one, kernel_one = args
    _, rows, cols, width = mixed_two.shape
    hidden = w_in_two.shape[0]
    pad = -(-cols // 16) * 16
    K, dp, space, Q = plan.chunks, plan.dp, plan.space, plan.piece
    R = space * Q
    F = dp * R
    E = 512
    tokens = rows * pad
    T = next(t for t in (256, pad) if tokens % t == 0)
    w_in_two = w_in_two.reshape(dp, K, R, width)
    w_out_two = w_out_two.reshape(dp, K, R, width)
    w_out_one = w_out_one.reshape(dp, K, R, width)

    def turned(x):
        return jnp.transpose(x, (0, 2, 1, 3))

    anywhere = pl.BlockSpec(memory_space=pl.ANY)
    vmem = pl.BlockSpec(memory_space=pltpu.VMEM)
    bits = plan.db + plan.sb
    piece_shapes = [
        pltpu.VMEM((K, 2) + (2,) * (bits - step) + (Q, lanes), BF16)
        for step in range(bits + 1)
        for lanes in plan.lanes
    ]
    token = pltpu.VMEM((rows, pad, width), BF16)
    flat = pltpu.VMEM((tokens, width), BF16)
    lying = pltpu.VMEM((cols, rows, width), BF16)
    raw = pltpu.VMEM((rows, cols, width), BF16)
    taps = kernel_two.shape[0]
    moves = plan.db + plan.sb
    dma = pltpu.SemaphoreType.DMA
    scratch = [
        lying, lying, lying, lying, raw,
        flat, flat, token,
        pltpu.VMEM((dp, K, R, width), BF16),
        pltpu.VMEM((dp, K, R, width), BF16),
        pltpu.VMEM((hidden, width), BF16),
        pltpu.VMEM((tokens // T, F, T), BF16),
        pltpu.VMEM((tokens // T, F, T), BF16),
        pltpu.VMEM((tokens, width), F32),
        raw,
        token,
        pltpu.VMEM((hidden // E, rows * pad, E), BF16),
        pltpu.VMEM((2, cols, width), BF16),
        pltpu.VMEM((2, cols, width), BF16),
        pltpu.VMEM((taps, width), F32),
        pltpu.VMEM((moves, taps, width), F32),
        pltpu.VMEM((K, space, 2, Q, width), BF16),
        *piece_shapes,
        dma((4,)), dma((2, K)), dma((2,)), dma((rows,)), dma((K,)),
        dma((K, plan.stages + 1, STREAMS)), dma((K, plan.stages + 1, STREAMS)),
        dma((K, plan.sb)), dma((K, plan.sb)),
        dma((2, 2)), dma((2, 2)), dma((moves,)), dma((moves,)),
    ]
    return pl.pallas_call(
        functools.partial(kernel, plan, (rows, cols, width), inv_batch),
        in_specs=[anywhere] * 5 + [vmem] + [anywhere] * 3 + [vmem],
        out_specs=[anywhere, anywhere, vmem],
        out_shape=[
            jax.ShapeDtypeStruct(mixed_two.shape, BF16),
            jax.ShapeDtypeStruct((K, space, 2, Q, width), BF16),
            jax.ShapeDtypeStruct((taps, width), F32),
        ],
        scratch_shapes=scratch,
        compiler_params=pltpu.CompilerParams(
            collective_id=0 if COMM else None, has_side_effects=True, vmem_limit_bytes=67_043_328
        ),
    )(
        turned(mixed_two), turned(input_two), turned(cotangent), w_in_two, w_out_two, kernel_two,
        turned(mixed_one), w_in_one, w_out_one, kernel_one,
    )


def shards(*args):
    dp, space = lax.axis_size("dp"), lax.axis_size("space")
    samples, width, hidden = args[0].shape[0], args[0].shape[3], args[3].shape[0]
    plan = Plan(dp, space, hidden, width)
    grad_one, grads, taps = whole_call(plan, 1.0 / (samples * dp), args)
    out = grads[:, :, 0].reshape(-1, width).astype(F32)
    inn = grads[:, :, 1].reshape(-1, width).astype(F32)
    return grad_one, inn, out, taps


def solution(mesh):
    tokens = P("dp", "space", None, None)
    return jax.shard_map(
        shards,
        mesh=mesh,
        in_specs=(tokens, tokens, tokens, P(), P(), P(), tokens, P(), P(), P()),
        out_specs=(tokens, P("dp", None), P("dp", None), P()),
        check_vma=False,
    )
```
